256 devices in a mesh: row: 4 (over x_hi, core), col: 4 (over y), pt: 16 (over x_lo, z).
Axes of the slice: x: 4 (x_hi: 2, x_lo: 2; x = x_hi * 2 + x_lo), y: 4, z: 8, core: 2. Of those that a mesh axis runs over, the one named last changes fastest.
Arguments:
- first_factors: int32 [32, 1024, 1024], P('pt', 'row', 'col'), may hold values from 0 to 12288
- second_factors: int32 [32, 1024, 1024], P('pt', 'row', 'col'), may hold values from 0 to 12288
Outputs:
- scaled_product: float32 [45, 1024, 1024], P(None, ('row', 'pt'), 'col')
The draws below stay inside these ranges and needn't reach their ends.
All inputs are finite; a program needn't handle non-finite values.
Results may differ from the reference program's by a relative error of at most 0.0003.
Values may be sent and summed in bfloat16 or wider, within the bound.
No kernel may reach another device: no remote copies, remote signals or barrier semaphores. Data moves between devices by JAX's collectives and lax.ppermute only.
A program may use at most 64 MiB of HBM per device.

```python
import jax
import jax.numpy as jnp
import numpy as np
from jax import lax

N = 1024
DEG = 16


def touch_ends(result, stream_key, low, top_value):
    place = [jax.random.randint(jax.random.fold_in(stream_key, axis), (), 0, length) for axis, length in enumerate(result.shape)]
    longest = result.shape.index(max(result.shape))
    neighbour = place[:longest] + [(place[longest] + 1) % result.shape[longest]] + place[longest + 1:]
    return result.at[tuple(place)].set(low).at[tuple(neighbour)].set(top_value)


def setup_inputs(seed: int = 0) -> dict:
    key_of = jax.random.split(jax.random.key(seed), 3)
    return {
        "first_factors": touch_ends(jax.random.randint(key_of[0], (2 * DEG, N, N), 0, 12289), jax.random.fold_in(key_of[0], 1), 0, 12288).astype(jnp.int32),
        "second_factors": touch_ends(jax.random.randint(key_of[1], (2 * DEG, N, N), 0, 12289), jax.random.fold_in(key_of[1], 1), 0, 12288).astype(jnp.int32),
    }


modulus = 12289
digit_base = 128


def primitive_root():
    for candidate in range(2, modulus):
        if pow(candidate, 6144, modulus) != 1 and pow(candidate, 4096, modulus) != 1:
            return candidate
    return 0


def make_table(order_size, row_count, column_count, inverse):
    generator = primitive_root()
    root_value = pow(generator, (modulus - 1) // order_size, modulus)
    scaling = 1
    if inverse:
        root_value = pow(root_value, modulus - 2, modulus)
        scaling = pow(order_size, modulus - 2, modulus)
    entries = [[pow(root_value, (row_index * column_index) % order_size, modulus) * scaling % modulus
                for column_index in range(column_count)] for row_index in range(row_count)]
    return np.array(entries, dtype=np.int64)


def exact_dot(left_part, right_part):
    return jnp.dot(left_part, right_part, precision=lax.Precision.HIGHEST, preferred_element_type=jnp.float32)


def value_digits(values):
    high_digit = values // digit_base
    return high_digit.astype(jnp.float32), (values - digit_base * high_digit).astype(jnp.float32)


def combine(high_high, high_low, low_high, low_low):
    top_part = high_high.astype(jnp.int32) % modulus
    middle_part = (high_low.astype(jnp.int32) + low_high.astype(jnp.int32)) % modulus
    return ((top_part * (digit_base * digit_base)) % modulus + middle_part * digit_base + low_low.astype(jnp.int32)) % modulus


def modular_product(matrix_table, values):
    table_high = jnp.asarray(matrix_table // digit_base, dtype=jnp.float32)
    table_low = jnp.asarray(matrix_table % digit_base, dtype=jnp.float32)
    data_high, data_low = value_digits(values)
    return combine(exact_dot(table_high, data_high), exact_dot(table_high, data_low),
                   exact_dot(table_low, data_high), exact_dot(table_low, data_low))


def transform(matrix_table, coefs):
    slot_count = coefs.shape[0]
    blocks = coefs.reshape(slot_count, 16, coefs.shape[1] // 16, coefs.shape[2]).transpose(1, 0, 2, 3)

    def one_block(block):
        flat_coefs = block.reshape(slot_count, -1)
        return modular_product(matrix_table, flat_coefs).reshape(-1, block.shape[1], block.shape[2])

    mapped = lax.map(one_block, blocks)
    return mapped.transpose(1, 0, 2, 3).reshape(-1, coefs.shape[1], coefs.shape[2])


def pointwise(left_values, right_values):
    def one_point(pair_in):
        left_high, left_low = value_digits(pair_in[0])
        right_high, right_low = value_digits(pair_in[1])
        return combine(exact_dot(left_high, right_high), exact_dot(left_high, right_low),
                       exact_dot(left_low, right_high), exact_dot(left_low, right_low))

    return lax.map(one_point, (left_values, right_values))


def reference(first_factors, second_factors):
    forward_one = make_table(2 * DEG, 2 * DEG, DEG, False)
    inverse_one = make_table(2 * DEG, 2 * DEG, 2 * DEG, True)
    forward_two = make_table(4 * DEG, 4 * DEG, 2 * DEG, False)
    inverse_two = make_table(4 * DEG, 3 * DEG - 3, 4 * DEG, True)
    left_values = jnp.concatenate([transform(forward_one, first_factors[:DEG]),
                                   transform(forward_one, first_factors[DEG:])], 0)
    right_values = jnp.concatenate([transform(forward_one, second_factors[:DEG]),
                                    transform(forward_one, second_factors[DEG:])], 0)
    products = pointwise(left_values, right_values)
    first_product = transform(inverse_one, products[:2 * DEG])
    second_product = transform(inverse_one, products[2 * DEG:])
    upper_values = transform(forward_two, first_product)
    lower_values = transform(forward_two[:, :DEG], second_product[DEG:])
    result_coefficients = transform(inverse_two, pointwise(upper_values, lower_values))
    return result_coefficients.astype(jnp.float32) / 12289.0
```

```python
import functools

import jax
import jax.numpy as jnp
import numpy as np
from jax import lax
from jax.experimental import pallas as pl
from jax.experimental.pallas import tpu as pltpu
from jax.sharding import PartitionSpec as P

DEG = 16
POINTS = 48
COEFS = 3 * DEG - 3

modulus = 12289
inverse_modulus = 1.0 / modulus


def primitive_root():
    for candidate in range(2, modulus):
        if pow(candidate, 6144, modulus) != 1 and pow(candidate, 4096, modulus) != 1:
            return candidate
    return 0


def powers(order, row_count, column_count, inverse=False):
    root = pow(primitive_root(), (modulus - 1) // order, modulus)
    scaling = 1
    if inverse:
        root = pow(root, modulus - 2, modulus)
        scaling = pow(order, modulus - 2, modulus)
    entries = [
        [pow(root, i * j % order, modulus) * scaling % modulus for j in range(column_count)]
        for i in range(row_count)
    ]
    return np.array(entries, dtype=np.int64)


def matrix_inverse(matrix):
    size = matrix.shape[0]
    work = np.concatenate([matrix % modulus, np.eye(size, dtype=np.int64)], axis=1)
    for k in range(size):
        pivot = k + int(np.nonzero(work[k:, k])[0][0])
        work[[k, pivot]] = work[[pivot, k]]
        work[k] = work[k] * pow(int(work[k, k]), modulus - 2, modulus) % modulus
        for i in range(size):
            if i != k:
                work[i] = (work[i] - work[i, k] * work[k]) % modulus
    return work[:, size:]


def centred(values):
    values = values % modulus
    return np.where(values > modulus // 2, values - modulus, values)


def table_digits(values):
    values = centred(values)
    high = (values + 64) >> 7
    return high, values - 128 * high


def expanded_table(matrix):
    of_high, of_low = table_digits(128 * matrix), table_digits(matrix)
    parts = np.stack([np.stack([of_high[k], of_low[k]], 0) for k in range(2)], 0)
    outputs, inputs = matrix.shape
    full = np.einsum("pdoi,rs->pordis", parts, np.eye(8, dtype=np.int64))
    return jnp.asarray(full.reshape(2 * outputs * 8, 2 * inputs * 8), dtype=jnp.bfloat16)


def reduced(value):
    return value - jnp.floor(value * inverse_modulus + 0.5) * float(modulus)


def mixed(table_ref, slots):
    inputs = slots.shape[0]
    half_rows = table_ref.shape[0] // 2
    outputs = half_rows // 8
    halves = []
    for h in range(2):
        part = slots[:, 8 * h : 8 * h + 8, :].reshape(inputs * 8, 256)
        high = (part + 64) >> 7
        low = part - (high << 7)
        digits = jnp.concatenate(
            [high.astype(jnp.float32).astype(jnp.bfloat16), low.astype(jnp.float32).astype(jnp.bfloat16)], 0
        )
        sums = jnp.dot(table_ref[...], digits, preferred_element_type=jnp.float32)
        top, bottom = sums[:half_rows], sums[half_rows:]
        quotient = jnp.floor(top * (128.0 * inverse_modulus) + bottom * inverse_modulus + 0.5)
        value = (top - 96.0 * quotient) * 128.0 + (bottom - quotient)
        halves.append(value.reshape(outputs, 8, 256))
    return jnp.concatenate(halves, axis=1)


def to_wire(value):
    return value.astype(jnp.int32).astype(jnp.int16)


def pack_kernel(first_ref, second_ref, out_ref):
    for a, ref in enumerate((first_ref, second_ref)):
        for b in range(2):
            out_ref[:, a, b] = ref[b].astype(jnp.int16).reshape(16, 16, 256)


def spread_kernel(table_ref, in_ref, out_ref):
    count = out_ref.shape[1] // 2
    for a in range(2):
        slots = in_ref[:, a].astype(jnp.int32).reshape(16, 16, 256)
        value = to_wire(mixed(table_ref, slots))
        out_ref[:, a * count : (a + 1) * count] = value.reshape(16, count, 16, 256)


def middle_kernel(table_ref, in_ref, out_ref):
    slots = in_ref[...].astype(jnp.int32).reshape(-1, 16, 256)
    out_ref[...] = to_wire(mixed(table_ref, slots)).reshape(out_ref.shape)


def final_kernel(table_ref, in_ref, out_ref):
    slots = in_ref[...].astype(jnp.int32).reshape(-1, 16, 256)
    value = mixed(table_ref, slots)
    value = jnp.where(value < 0.0, value + float(modulus), value)
    out_ref[...] = value / float(modulus)


def product_kernel(shift_ref, *refs):
    left_refs, right_refs, out_ref = refs[:4], refs[4:8], refs[8]
    left_scratch, right_scratch = refs[9:12], refs[12:15]
    shift = shift_ref[0]

    def store_digits(piece, scratch, place):
        value = piece.astype(jnp.int32).reshape(256, 256)
        high = (value + 64) >> 7
        low = value - (high << 7)
        both = high + low
        for part, ref in zip((high, low, both), scratch):
            ref[place] = part.astype(jnp.float32).astype(jnp.bfloat16)

    for j in range(out_ref.shape[1]):
        for m in range(4):
            store_digits(left_refs[m][:, j], left_scratch, (slice(None), slice(256 * m, 256 * m + 256)))
            block = pl.multiple_of((m ^ shift) * 256, 256)
            store_digits(right_refs[m][:, j], right_scratch, (pl.ds(block, 256), slice(None)))
        high_high, low_low, both_both = (
            jnp.dot(left[...], right[...], preferred_element_type=jnp.float32)
            for left, right in zip(left_scratch, right_scratch)
        )
        value = reduced(high_high) * 128.0 + (both_both - high_high - low_low)
        value = reduced(reduced(value) * 128.0 + low_low)
        out_ref[:, j] = to_wire(value).reshape(16, 16, 256)


def whole(shape):
    return pl.BlockSpec(shape, lambda i: (0,) * len(shape))


def params():
    return pltpu.CompilerParams(dimension_semantics=("arbitrary",), vmem_limit_bytes=24 * 1024 * 1024)


def cost(flops):
    return pl.CostEstimate(flops=flops, bytes_accessed=1 << 20, transcendentals=0)


def pack(first, second):
    return pl.pallas_call(
        pack_kernel,
        grid=(1,),
        out_shape=jax.ShapeDtypeStruct((16, 2, 2, 16, 256), jnp.int16),
        in_specs=[whole((2, 256, 256))] * 2,
        out_specs=whole((16, 2, 2, 16, 256)),
        compiler_params=params(),
        cost_estimate=cost(1 << 20),
        name="pack",
    )(first, second)


def spread(table, entries, pair, name):
    count = table.shape[0] // 256
    out_shape = (16, 2 * count, 16, 256)
    return pl.pallas_call(
        spread_kernel,
        grid=(1,),
        out_shape=jax.ShapeDtypeStruct(out_shape, jnp.int16),
        in_specs=[whole(table.shape), pl.BlockSpec((8, 2, 2, 16, 256), lambda i: (pair, 0, 0, 0, 0))],
        out_specs=whole(out_shape),
        compiler_params=params(),
        cost_estimate=cost(4 * 2 * table.shape[0] * table.shape[1] * 256),
        name=name,
    )(table, entries)


def middle(table, values):
    out_shape = (16, POINTS // 16, 16, 256)
    return pl.pallas_call(
        middle_kernel,
        grid=(1,),
        out_shape=jax.ShapeDtypeStruct(out_shape, jnp.int16),
        in_specs=[whole(table.shape), whole(values.shape)],
        out_specs=whole(out_shape),
        compiler_params=params(),
        cost_estimate=cost(2 * 2 * table.shape[0] * table.shape[1] * 256),
        name="middle",
    )(table, values)


def final(table, values):
    out_shape = (COEFS, 16, 256)
    return pl.pallas_call(
        final_kernel,
        grid=(1,),
        out_shape=jax.ShapeDtypeStruct(out_shape, jnp.float32),
        in_specs=[whole(table.shape), whole(values.shape)],
        out_specs=whole(out_shape),
        compiler_params=params(),
        cost_estimate=cost(2 * 2 * table.shape[0] * table.shape[1] * 256),
        name="final",
    )(table, values)


def product(shift, left, right, name):
    shape = left[0].shape
    return pl.pallas_call(
        product_kernel,
        grid=(1,),
        out_shape=jax.ShapeDtypeStruct(shape, jnp.int16),
        in_specs=[pl.BlockSpec(memory_space=pltpu.SMEM)] + [whole(shape)] * 8,
        out_specs=whole(shape),
        scratch_shapes=[pltpu.VMEM((256, 1024), jnp.bfloat16)] * 3 + [pltpu.VMEM((1024, 256), jnp.bfloat16)] * 3,
        compiler_params=params(),
        cost_estimate=cost(shape[1] * 3 * 2 * 256 * 256 * 1024),
        name=name,
    )(shift, *left, *right)


def exchange(value):
    return lax.all_to_all(value, "pt", split_axis=0, concat_axis=0, tiled=True)


def swapped(value, axis, bits):
    return lax.ppermute(value, axis, [(i, i ^ bits) for i in range(4)])


def along_columns(value):
    return [value] + [swapped(value, "col", m) for m in (1, 2, 3)]


def along_rows(value):
    across = swapped(value, "row", 2)
    return [value, swapped(value, "row", 1), across, swapped(across, "row", 1)]


def local(first_factors, second_factors):
    forward_two = powers(4 * DEG, POINTS, 2 * DEG)
    spread_one = expanded_table(powers(2 * DEG, 2 * DEG, DEG))
    spread_two = expanded_table(forward_two[:, :DEG])
    lift = forward_two[:, :DEG] @ powers(2 * DEG, 2 * DEG, 2 * DEG, True)[DEG:] % modulus
    back = matrix_inverse(powers(4 * DEG, POINTS, POINTS))[:COEFS]
    shift = (lax.axis_index("row") ^ lax.axis_index("col")).astype(jnp.int32).reshape(1)

    entries = exchange(pack(first_factors, second_factors))
    at_one = exchange(spread(spread_one, entries, 1, "spread_one"))
    to_two = spread(spread_two, entries, 0, "spread_two")
    left_one, right_one = along_columns(at_one[:, :2]), along_rows(at_one[:, 2:])
    to_two, at_one = lax.optimization_barrier((to_two, at_one))
    at_two = exchange(to_two)
    products_one = product(shift, left_one, right_one, "product_one")
    products_one, at_two = lax.optimization_barrier((products_one, at_two))
    returned = exchange(products_one)
    left_two, right_two = along_columns(at_two[:, :3]), along_rows(at_two[:, 3:])
    upper = along_columns(product(shift, left_two, right_two, "product_upper"))
    to_lower = middle(expanded_table(lift), returned)
    lower = along_rows(exchange(to_lower))
    products_two = exchange(product(shift, upper_in_rows(upper), lower, "product_two"))
    return final(expanded_table(back), products_two)


def upper_in_rows(upper):
    return upper


def solution(mesh):
    in_specs = (P("pt", "row", "col"), P("pt", "row", "col"))
    out_specs = P(None, ("row", "pt"), "col")
    return jax.shard_map(local, mesh=mesh, in_specs=in_specs, out_specs=out_specs, check_vma=False)
```

```python
import jax
import jax.numpy as jnp
import numpy as np
from jax import lax
from jax.experimental import pallas as pl
from jax.experimental.pallas import tpu as pltpu
from jax.sharding import PartitionSpec as P

DEG = 16
POINTS = 48
COEFS = 3 * DEG - 3

modulus = 12289
inverse_modulus = 1.0 / modulus


def primitive_root():
    for candidate in range(2, modulus):
        if pow(candidate, 6144, modulus) != 1 and pow(candidate, 4096, modulus) != 1:
            return candidate
    return 0


def powers(order, row_count, column_count, inverse=False):
    root = pow(primitive_root(), (modulus - 1) // order, modulus)
    scaling = 1
    if inverse:
        root = pow(root, modulus - 2, modulus)
        scaling = pow(order, modulus - 2, modulus)
    entries = [
        [pow(root, i * j % order, modulus) * scaling % modulus for j in range(column_count)]
        for i in range(row_count)
    ]
    return np.array(entries, dtype=np.int64)


def matrix_inverse(matrix):
    size = matrix.shape[0]
    work = np.concatenate([matrix % modulus, np.eye(size, dtype=np.int64)], axis=1)
    for k in range(size):
        pivot = k + int(np.nonzero(work[k:, k])[0][0])
        work[[k, pivot]] = work[[pivot, k]]
        work[k] = work[k] * pow(int(work[k, k]), modulus - 2, modulus) % modulus
        for i in range(size):
            if i != k:
                work[i] = (work[i] - work[i, k] * work[k]) % modulus
    return work[:, size:]


def centred(values):
    values = values % modulus
    return np.where(values > modulus // 2, values - modulus, values)


def table_digits(values):
    values = centred(values)
    high = (values + 64) >> 7
    return high, values - 128 * high


def digit_table(matrix):
    of_high, of_low = table_digits(128 * matrix), table_digits(matrix)
    parts = [np.concatenate([of_high[k], of_low[k]], 1) for k in range(2)]
    return jnp.asarray(np.concatenate(parts, 0), dtype=jnp.bfloat16)


def expanded(table_ref):
    rows, columns = table_ref.shape
    wide = (columns, 8 * columns)
    place = lax.broadcasted_iota(jnp.int32, wide, 1) // 8 == lax.broadcasted_iota(jnp.int32, wide, 0)
    spread = jnp.dot(table_ref[...], place.astype(jnp.bfloat16), preferred_element_type=jnp.float32)
    full = (rows, 8, 8 * columns)
    same = lax.broadcasted_iota(jnp.int32, full, 2) % 8 == lax.broadcasted_iota(jnp.int32, full, 1)
    table = jnp.where(same, jnp.broadcast_to(spread[:, None, :], full), 0.0)
    return table.reshape(8 * rows, 8 * columns).astype(jnp.bfloat16)


def reduced(value):
    return value - jnp.floor(value * inverse_modulus + 0.5) * float(modulus)


def mixed(table, slots):
    inputs = slots.shape[0]
    half_rows = table.shape[0] // 2
    outputs = half_rows // 8
    halves = []
    for h in range(2):
        digits = jnp.concatenate(digits_of(slots[:, 8 * h : 8 * h + 8, :].reshape(inputs * 8, 256)), 0)
        sums = jnp.dot(table, digits, preferred_element_type=jnp.float32)
        top, bottom = sums[:half_rows], sums[half_rows:]
        quotient = jnp.floor(top * (128.0 * inverse_modulus) + bottom * inverse_modulus + 0.5)
        value = (top - 96.0 * quotient) * 128.0 + (bottom - quotient)
        halves.append(value.reshape(outputs, 8, 256))
    return jnp.concatenate(halves, axis=1)


def digits_of(wire):
    wire = wire.astype(jnp.int32)
    high = (wire >> 7).astype(jnp.float32).astype(jnp.bfloat16)
    low = (wire & 127).astype(jnp.float32).astype(jnp.bfloat16)
    return high, low - jnp.asarray(64.0, jnp.bfloat16)


def to_wire(value):
    return (value + 64.0).astype(jnp.int32).astype(jnp.int16)


def part_kernel(in_ref, left_ref, right_ref):
    count = left_ref.shape[1]
    left_ref[...] = in_ref[:, :count]
    right_ref[...] = in_ref[:, count:]


def spread_kernel(table_ref, in_ref, out_ref):
    count = out_ref.shape[1] // 2
    table = expanded(table_ref)
    for a in range(2):
        slots = in_ref[:, a].astype(jnp.int32).reshape(16, 16, 256)
        value = to_wire(mixed(table, slots))
        out_ref[:, a * count : (a + 1) * count] = value.reshape(16, count, 16, 256)


def middle_kernel(table_ref, in_ref, out_ref):
    slots = in_ref[...].astype(jnp.int32).reshape(-1, 16, 256)
    out_ref[...] = to_wire(mixed(expanded(table_ref), slots)).reshape(out_ref.shape)


def final_kernel(table_ref, in_ref, out_ref):
    slots = in_ref[...].astype(jnp.int32).reshape(-1, 16, 256)
    value = mixed(expanded(table_ref), slots)[:COEFS]
    value = jnp.where(value < 0.0, value + float(modulus), value)
    out_ref[...] = value / float(modulus)


def product_kernel(shift_ref, *refs):
    left_refs, right_refs, out_ref = refs[:4], refs[4:8], refs[8]
    shift = shift_ref[0]

    def store_digits(piece, scratch, place):
        high, low = digits_of(piece.reshape(256, 256))
        for part, ref in zip((high, low, high + low), scratch):
            ref[place] = part

    for j in range(out_ref.shape[1]):
        left_scratch, right_scratch = ([ref.at[j] for ref in refs[k : k + 3]] for k in (9, 12))
        for m in range(4):
            store_digits(left_refs[m][:, j], left_scratch, (slice(None), slice(256 * m, 256 * m + 256)))
            block = pl.multiple_of((m ^ shift) * 256, 256)
            store_digits(right_refs[m][:, j], right_scratch, (pl.ds(block, 256), slice(None)))
        high_high, low_low, both_both = (
            jnp.dot(left[...], right[...], preferred_element_type=jnp.float32)
            for left, right in zip(left_scratch, right_scratch)
        )
        value = reduced(high_high) * 128.0 + (both_both - high_high - low_low)
        value = reduced(reduced(value) * 128.0 + low_low)
        out_ref[:, j] = to_wire(value).reshape(16, 16, 256)


def whole(shape):
    return pl.BlockSpec(shape, lambda i: (0,) * len(shape))


def params(mebibytes=12):
    return pltpu.CompilerParams(dimension_semantics=("arbitrary",), vmem_limit_bytes=mebibytes * 1024 * 1024)


def cost(flops):
    return pl.CostEstimate(flops=flops // 8, bytes_accessed=1 << 16, transcendentals=0)


def pack(first, second):
    both = [(value + 64).astype(jnp.int16).reshape(2, 16, 16, 256) for value in (first, second)]
    return jnp.stack(both).transpose(2, 0, 1, 3, 4)


def parted(both):
    shape = both.shape[:1] + (both.shape[1] // 2,) + both.shape[2:]
    return pl.pallas_call(
        part_kernel,
        grid=(1,),
        out_shape=[jax.ShapeDtypeStruct(shape, jnp.int16)] * 2,
        in_specs=[whole(both.shape)],
        out_specs=[whole(shape)] * 2,
        compiler_params=params(4),
        cost_estimate=cost(1 << 20),
    )(both)


def spread(table, entries, pair):
    count = table.shape[0] // 32
    out_shape = (16, 2 * count, 16, 256)
    return pl.pallas_call(
        spread_kernel,
        grid=(1,),
        out_shape=jax.ShapeDtypeStruct(out_shape, jnp.int16),
        in_specs=[whole(table.shape), pl.BlockSpec((8, 2, 2, 16, 256), lambda i: (pair, 0, 0, 0, 0))],
        out_specs=whole(out_shape),
        compiler_params=params(),
        cost_estimate=cost(4 * 2 * 64 * table.shape[0] * table.shape[1] * 256),
    )(table, entries)


def middle(table, values):
    out_shape = (16, POINTS // 16, 16, 256)
    return pl.pallas_call(
        middle_kernel,
        grid=(1,),
        out_shape=jax.ShapeDtypeStruct(out_shape, jnp.int16),
        in_specs=[whole(table.shape), whole(values.shape)],
        out_specs=whole(out_shape),
        compiler_params=params(),
        cost_estimate=cost(2 * 2 * 64 * table.shape[0] * table.shape[1] * 256),
        name="middle",
    )(table, values)


def final(table, values):
    out_shape = (COEFS, 16, 256)
    return pl.pallas_call(
        final_kernel,
        grid=(1,),
        out_shape=jax.ShapeDtypeStruct(out_shape, jnp.float32),
        in_specs=[whole(table.shape), whole(values.shape)],
        out_specs=whole(out_shape),
        compiler_params=params(),
        cost_estimate=cost(2 * 2 * 64 * table.shape[0] * table.shape[1] * 256),
        name="final",
    )(table, values)


def product(shift, left, right):
    shape = left[0].shape
    return pl.pallas_call(
        product_kernel,
        grid=(1,),
        out_shape=jax.ShapeDtypeStruct(shape, jnp.int16),
        in_specs=[pl.BlockSpec(memory_space=pltpu.SMEM)] + [whole(shape)] * 8,
        out_specs=whole(shape),
        scratch_shapes=[pltpu.VMEM((shape[1], 256, 1024), jnp.bfloat16)] * 3
        + [pltpu.VMEM((shape[1], 1024, 256), jnp.bfloat16)] * 3,
        compiler_params=params(20),
        cost_estimate=cost(shape[1] * 3 * 2 * 256 * 256 * 1024),
    )(shift, *left, *right)


def exchange(value):
    return lax.all_to_all(value, "pt", split_axis=0, concat_axis=0, tiled=True)


def swapped(value, axis, bits):
    return lax.ppermute(value, axis, [(i, i ^ bits) for i in range(4)])


def along_columns(value):
    return [value] + [swapped(value, "col", m) for m in (1, 2, 3)]


def along_rows(value):
    across = swapped(value, "row", 2)
    return [value, swapped(value, "row", 1), across, swapped(across, "row", 1)]


def local(first_factors, second_factors):
    forward_two = powers(4 * DEG, POINTS, 2 * DEG)
    spread_one = digit_table(powers(2 * DEG, 2 * DEG, DEG))
    spread_two = digit_table(forward_two[:, :DEG])
    lift = forward_two[:, :DEG] @ powers(2 * DEG, 2 * DEG, 2 * DEG, True)[DEG:] % modulus
    back = matrix_inverse(powers(4 * DEG, POINTS, POINTS))
    shift = (lax.axis_index("row") ^ lax.axis_index("col")).astype(jnp.int32).reshape(1)

    entries = exchange(pack(first_factors, second_factors))
    at_one = exchange(spread(spread_one, entries, 1))
    to_two = spread(spread_two, entries, 0)
    left_one, right_one = parted(at_one)
    left_one, right_one = along_columns(left_one), along_rows(right_one)
    to_two, at_one = lax.optimization_barrier((to_two, at_one))
    at_two = exchange(to_two)
    products_one = product(shift, left_one, right_one)
    products_one, at_two = lax.optimization_barrier((products_one, at_two))
    returned = exchange(products_one)
    left_two, right_two = parted(at_two)
    left_two, right_two = along_columns(left_two), along_rows(right_two)
    to_lower = middle(digit_table(lift), returned)
    upper = along_columns(product(shift, left_two, right_two))
    lower = along_rows(exchange(to_lower))
    products_two = exchange(product(shift, upper, lower))
    return final(digit_table(back), products_two)


def solution(mesh):
    in_specs = (P("pt", "row", "col"), P("pt", "row", "col"))
    out_specs = P(None, ("row", "pt"), "col")
    return jax.shard_map(local, mesh=mesh, in_specs=in_specs, out_specs=out_specs, check_vma=False)
```

```python
import jax
import jax.numpy as jnp
import numpy as np
from jax import lax
from jax.experimental import pallas as pl
from jax.experimental.pallas import tpu as pltpu
from jax.sharding import PartitionSpec as P

DEG = 16
POINTS = 48
COEFS = 3 * DEG - 3

modulus = 12289
inverse_modulus = 1.0 / modulus


def primitive_root():
    for candidate in range(2, modulus):
        if pow(candidate, 6144, modulus) != 1 and pow(candidate, 4096, modulus) != 1:
            return candidate
    return 0


def powers(order, row_count, column_count, inverse=False):
    root = pow(primitive_root(), (modulus - 1) // order, modulus)
    scaling = 1
    if inverse:
        root = pow(root, modulus - 2, modulus)
        scaling = pow(order, modulus - 2, modulus)
    entries = [
        [pow(root, i * j % order, modulus) * scaling % modulus for j in range(column_count)]
        for i in range(row_count)
    ]
    return np.array(entries, dtype=np.int64)


def matrix_inverse(matrix):
    size = matrix.shape[0]
    work = np.concatenate([matrix % modulus, np.eye(size, dtype=np.int64)], axis=1)
    for k in range(size):
        pivot = k + int(np.nonzero(work[k:, k])[0][0])
        work[[k, pivot]] = work[[pivot, k]]
        work[k] = work[k] * pow(int(work[k, k]), modulus - 2, modulus) % modulus
        for i in range(size):
            if i != k:
                work[i] = (work[i] - work[i, k] * work[k]) % modulus
    return work[:, size:]


def centred(values):
    values = values % modulus
    return np.where(values > modulus // 2, values - modulus, values)


def table_digits(values):
    values = centred(values)
    high = (values + 64) >> 7
    return high, values - 128 * high


def digit_table(matrix):
    of_high, of_low = table_digits(128 * matrix), table_digits(matrix)
    parts = [np.concatenate([of_high[k], of_low[k]], 1) for k in range(2)]
    return jnp.asarray(np.concatenate(parts, 0), dtype=jnp.bfloat16)


def expanded(table_ref):
    rows, columns = table_ref.shape
    wide = (columns, 8 * columns)
    place = lax.broadcasted_iota(jnp.int32, wide, 1) // 8 == lax.broadcasted_iota(jnp.int32, wide, 0)
    spread = jnp.dot(table_ref[...], place.astype(jnp.bfloat16), preferred_element_type=jnp.float32)
    full = (rows, 8, 8 * columns)
    same = lax.broadcasted_iota(jnp.int32, full, 2) % 8 == lax.broadcasted_iota(jnp.int32, full, 1)
    table = jnp.where(same, jnp.broadcast_to(spread[:, None, :], full), 0.0)
    return table.reshape(8 * rows, 8 * columns).astype(jnp.bfloat16)


def reduced(value):
    return value - jnp.floor(value * inverse_modulus + 0.5) * float(modulus)


def mixed(table, slots):
    inputs = slots.shape[0]
    half_rows = table.shape[0] // 2
    outputs = half_rows // 8
    halves = []
    for h in range(2):
        digits = jnp.concatenate(digits_of(slots[:, 8 * h : 8 * h + 8, :].reshape(inputs * 8, 256)), 0)
        sums = jnp.dot(table, digits, preferred_element_type=jnp.float32)
        top, bottom = sums[:half_rows], sums[half_rows:]
        quotient = jnp.floor(top * (128.0 * inverse_modulus) + bottom * inverse_modulus + 0.5)
        value = (top - 96.0 * quotient) * 128.0 + (bottom - quotient)
        halves.append(value.reshape(outputs, 8, 256))
    return jnp.concatenate(halves, axis=1)


def digits_of(wire):
    wire = wire.astype(jnp.int32)
    high = (wire >> 7).astype(jnp.float32).astype(jnp.bfloat16)
    low = (wire & 127).astype(jnp.float32).astype(jnp.bfloat16)
    return high, low - jnp.asarray(64.0, jnp.bfloat16)


def to_wire(value):
    return (value + 64.0).astype(jnp.int32).astype(jnp.int16)


def part_kernel(in_ref, left_ref, right_ref):
    count = left_ref.shape[1]
    left_ref[...] = in_ref[:, :count]
    right_ref[...] = in_ref[:, count:]


def spread_kernel(table_ref, in_ref, out_ref):
    count = out_ref.shape[1] // 2
    table = expanded(table_ref)
    for a in range(2):
        slots = in_ref[:, a].astype(jnp.int32).reshape(16, 16, 256)
        value = to_wire(mixed(table, slots))
        out_ref[:, a * count : (a + 1) * count] = value.reshape(16, count, 16, 256)


def middle_kernel(table_ref, in_ref, out_ref):
    slots = in_ref[...].astype(jnp.int32).reshape(-1, 16, 256)
    out_ref[...] = to_wire(mixed(expanded(table_ref), slots)).reshape(out_ref.shape)


def final_kernel(table_ref, in_ref, out_ref):
    slots = in_ref[...].astype(jnp.int32).reshape(-1, 16, 256)
    value = mixed(expanded(table_ref), slots)[:COEFS]
    value = jnp.where(value < 0.0, value + float(modulus), value)
    out_ref[...] = value / float(modulus)


def product_kernel(shift_ref, *refs):
    left_refs, right_refs, out_ref = refs[:4], refs[4:8], refs[8]
    shift = shift_ref[0]

    def store_digits(piece, scratch, place):
        high, low = digits_of(piece.reshape(256, 256))
        for part, ref in zip((high, low, high + low), scratch):
            ref[place] = part

    for j in range(out_ref.shape[1]):
        left_scratch, right_scratch = ([ref.at[j] for ref in refs[k : k + 3]] for k in (9, 12))
        for m in range(4):
            store_digits(left_refs[m][:, j], left_scratch, (slice(None), slice(256 * m, 256 * m + 256)))
            block = pl.multiple_of((m ^ shift) * 256, 256)
            store_digits(right_refs[m][:, j], right_scratch, (pl.ds(block, 256), slice(None)))
        high_high, low_low, both_both = (
            jnp.dot(left[...], right[...], preferred_element_type=jnp.float32)
            for left, right in zip(left_scratch, right_scratch)
        )
        value = reduced(high_high) * 128.0 + (both_both - high_high - low_low)
        value = reduced(reduced(value) * 128.0 + low_low)
        out_ref[:, j] = to_wire(value).reshape(16, 16, 256)


def whole(shape):
    return pl.BlockSpec(shape, lambda i: (0,) * len(shape))


def params(mebibytes=12):
    return pltpu.CompilerParams(dimension_semantics=("arbitrary",), vmem_limit_bytes=mebibytes * 1024 * 1024)


def cost(flops):
    return pl.CostEstimate(flops=flops // 8, bytes_accessed=1 << 16, transcendentals=0)


def pack(first, second):
    both = [(value + 64).astype(jnp.int16).reshape(2, 16, 16, 256) for value in (first, second)]
    return jnp.stack(both).transpose(2, 0, 1, 3, 4)


def parted(both):
    shape = both.shape[:1] + (both.shape[1] // 2,) + both.shape[2:]
    return pl.pallas_call(
        part_kernel,
        grid=(1,),
        out_shape=[jax.ShapeDtypeStruct(shape, jnp.int16)] * 2,
        in_specs=[whole(both.shape)],
        out_specs=[whole(shape)] * 2,
        compiler_params=params(4),
        cost_estimate=cost(1 << 20),
    )(both)


def spread(table, entries, pair):
    count = table.shape[0] // 32
    out_shape = (16, 2 * count, 16, 256)
    return pl.pallas_call(
        spread_kernel,
        grid=(1,),
        out_shape=jax.ShapeDtypeStruct(out_shape, jnp.int16),
        in_specs=[whole(table.shape), pl.BlockSpec((8, 2, 2, 16, 256), lambda i: (pair, 0, 0, 0, 0))],
        out_specs=whole(out_shape),
        compiler_params=params(),
        cost_estimate=cost(4 * 2 * 64 * table.shape[0] * table.shape[1] * 256),
    )(table, entries)


def middle(table, values):
    out_shape = (16, POINTS // 16, 16, 256)
    return pl.pallas_call(
        middle_kernel,
        grid=(1,),
        out_shape=jax.ShapeDtypeStruct(out_shape, jnp.int16),
        in_specs=[whole(table.shape), whole(values.shape)],
        out_specs=whole(out_shape),
        compiler_params=params(),
        cost_estimate=cost(2 * 2 * 64 * table.shape[0] * table.shape[1] * 256),
        name="middle",
    )(table, values)


def final(table, values):
    out_shape = (COEFS, 16, 256)
    return pl.pallas_call(
        final_kernel,
        grid=(1,),
        out_shape=jax.ShapeDtypeStruct(out_shape, jnp.float32),
        in_specs=[whole(table.shape), whole(values.shape)],
        out_specs=whole(out_shape),
        compiler_params=params(),
        cost_estimate=cost(2 * 2 * 64 * table.shape[0] * table.shape[1] * 256),
        name="final",
    )(table, values)


def product(shift, left, right, aliases):
    shape = left[0].shape
    return pl.pallas_call(
        product_kernel,
        grid=(1,),
        out_shape=jax.ShapeDtypeStruct(shape, jnp.int16),
        in_specs=[pl.BlockSpec(memory_space=pltpu.SMEM)] + [whole(shape)] * 8,
        out_specs=whole(shape),
        scratch_shapes=[pltpu.VMEM((shape[1], 256, 1024), jnp.bfloat16)] * 3
        + [pltpu.VMEM((shape[1], 1024, 256), jnp.bfloat16)] * 3,
        input_output_aliases=aliases,
        compiler_params=params(20),
        cost_estimate=cost(shape[1] * 3 * 2 * 256 * 256 * 1024),
    )(shift, *left, *right)


def exchange(value):
    return lax.all_to_all(value, "pt", split_axis=0, concat_axis=0, tiled=True)


def swapped(value, axis, bits):
    return lax.ppermute(value, axis, [(i, i ^ bits) for i in range(4)])


def along_columns(value):
    return [value] + [swapped(value, "col", m) for m in (1, 2, 3)]


def along_rows(value):
    across = swapped(value, "row", 2)
    return [value, swapped(value, "row", 1), across, swapped(across, "row", 1)]


def local(first_factors, second_factors):
    forward_two = powers(4 * DEG, POINTS, 2 * DEG)
    spread_one = digit_table(powers(2 * DEG, 2 * DEG, DEG))
    spread_two = digit_table(forward_two[:, :DEG])
    lift = forward_two[:, :DEG] @ powers(2 * DEG, 2 * DEG, 2 * DEG, True)[DEG:] % modulus
    back = matrix_inverse(powers(4 * DEG, POINTS, POINTS))
    shift = (lax.axis_index("row") ^ lax.axis_index("col")).astype(jnp.int32).reshape(1)

    entries = exchange(pack(first_factors, second_factors))
    at_one = exchange(spread(spread_one, entries, 1))
    to_two = spread(spread_two, entries, 0)
    left_one, right_one = parted(at_one)
    left_one, right_one = along_columns(left_one), along_rows(right_one)
    to_two, at_one = lax.optimization_barrier((to_two, at_one))
    at_two = exchange(to_two)
    products_one = product(shift, left_one, right_one, {})
    products_one, at_two = lax.optimization_barrier((products_one, at_two))
    returned = exchange(products_one)
    left_two, right_two = parted(at_two)
    left_two, right_two = along_columns(left_two), along_rows(right_two)
    to_lower = middle(digit_table(lift), returned)
    upper = along_columns(product(shift, left_two, right_two, {1: 0}))
    lower = along_rows(exchange(to_lower))
    products_two = exchange(product(shift, upper, lower, {1: 0}))
    return final(digit_table(back), products_two)


def solution(mesh):
    in_specs = (P("pt", "row", "col"), P("pt", "row", "col"))
    out_specs = P(None, ("row", "pt"), "col")
    return jax.shard_map(local, mesh=mesh, in_specs=in_specs, out_specs=out_specs, check_vma=False)
```

```python
import jax
import jax.numpy as jnp
import numpy as np
from jax import lax
from jax.experimental import pallas as pl
from jax.experimental.pallas import tpu as pltpu
from jax.sharding import PartitionSpec as P

DEG = 16
POINTS = 48
COEFS = 3 * DEG - 3

modulus = 12289
inverse_modulus = 1.0 / modulus


def primitive_root():
    for candidate in range(2, modulus):
        if pow(candidate, 6144, modulus) != 1 and pow(candidate, 4096, modulus) != 1:
            return candidate
    return 0


def powers(order, row_count, column_count, inverse=False):
    root = pow(primitive_root(), (modulus - 1) // order, modulus)
    scaling = 1
    if inverse:
        root = pow(root, modulus - 2, modulus)
        scaling = pow(order, modulus - 2, modulus)
    entries = [
        [pow(root, i * j % order, modulus) * scaling % modulus for j in range(column_count)]
        for i in range(row_count)
    ]
    return np.array(entries, dtype=np.int64)


def matrix_inverse(matrix):
    size = matrix.shape[0]
    work = np.concatenate([matrix % modulus, np.eye(size, dtype=np.int64)], axis=1)
    for k in range(size):
        pivot = k + int(np.nonzero(work[k:, k])[0][0])
        work[[k, pivot]] = work[[pivot, k]]
        work[k] = work[k] * pow(int(work[k, k]), modulus - 2, modulus) % modulus
        for i in range(size):
            if i != k:
                work[i] = (work[i] - work[i, k] * work[k]) % modulus
    return work[:, size:]


def centred(values):
    values = values % modulus
    return np.where(values > modulus // 2, values - modulus, values)


def table_digits(values):
    values = centred(values)
    high = (values + 64) >> 7
    return high, values - 128 * high


def digit_table(matrix):
    of_high, of_low = table_digits(128 * matrix), table_digits(matrix)
    parts = [np.concatenate([of_high[k], of_low[k]], 1) for k in range(2)]
    return jnp.asarray(np.concatenate(parts, 0), dtype=jnp.bfloat16)


def expanded(table_ref):
    rows, columns = table_ref.shape
    wide = (columns, 8 * columns)
    place = lax.broadcasted_iota(jnp.int32, wide, 1) // 8 == lax.broadcasted_iota(jnp.int32, wide, 0)
    spread = jnp.dot(table_ref[...], place.astype(jnp.bfloat16), preferred_element_type=jnp.float32)
    full = (rows, 8, 8 * columns)
    same = lax.broadcasted_iota(jnp.int32, full, 2) % 8 == lax.broadcasted_iota(jnp.int32, full, 1)
    table = jnp.where(same, jnp.broadcast_to(spread[:, None, :], full), 0.0)
    return table.reshape(8 * rows, 8 * columns).astype(jnp.bfloat16)


def reduced(value):
    return value - jnp.floor(value * inverse_modulus + 0.5) * float(modulus)


def mixed(table, slots):
    inputs = slots.shape[0]
    half_rows = table.shape[0] // 2
    outputs = half_rows // 8
    halves = []
    for h in range(2):
        digits = jnp.concatenate(digits_of(slots[:, 8 * h : 8 * h + 8, :].reshape(inputs * 8, 256)), 0)
        sums = jnp.dot(table, digits, preferred_element_type=jnp.float32)
        top, bottom = sums[:half_rows], sums[half_rows:]
        quotient = jnp.floor(top * (128.0 * inverse_modulus) + bottom * inverse_modulus + 0.5)
        value = (top - 96.0 * quotient) * 128.0 + (bottom - quotient)
        halves.append(value.reshape(outputs, 8, 256))
    return jnp.concatenate(halves, axis=1)


def digits_of(wire):
    wire = wire.astype(jnp.int32)
    high = (wire >> 7).astype(jnp.float32).astype(jnp.bfloat16)
    low = (wire & 127).astype(jnp.float32).astype(jnp.bfloat16)
    return high, low - jnp.asarray(64.0, jnp.bfloat16)


def to_wire(value):
    return (value + 64.0).astype(jnp.int32).astype(jnp.int16)


def part_kernel(in_ref, left_ref, right_ref):
    count = left_ref.shape[1]
    left_ref[...] = in_ref[:, :count]
    right_ref[...] = in_ref[:, count:]


def spread_kernel(table_ref, in_ref, out_ref):
    count = out_ref.shape[1] // 2
    table = expanded(table_ref)
    for a in range(2):
        slots = in_ref[:, a].astype(jnp.int32).reshape(16, 16, 256)
        value = to_wire(mixed(table, slots))
        out_ref[:, a * count : (a + 1) * count] = value.reshape(16, count, 16, 256)


def middle_kernel(table_ref, in_ref, out_ref):
    slots = in_ref[...].astype(jnp.int32).reshape(-1, 16, 256)
    out_ref[...] = to_wire(mixed(expanded(table_ref), slots)).reshape(out_ref.shape)


def final_kernel(table_ref, in_ref, out_ref):
    slots = in_ref[...].astype(jnp.int32).reshape(-1, 16, 256)
    value = mixed(expanded(table_ref), slots)[:COEFS]
    value = jnp.where(value < 0.0, value + float(modulus), value)
    out_ref[...] = value / float(modulus)


def product_kernel(shift_ref, *refs):
    left_refs, right_refs, out_ref = refs[:4], refs[4:8], refs[8]
    shift = shift_ref[0]

    def store_digits(piece, scratch, place):
        high, low = digits_of(piece.reshape(256, 256))
        for part, ref in zip((high, low), scratch):
            ref[place] = part

    for j in range(out_ref.shape[1]):
        left_scratch, right_scratch = ([ref.at[j] for ref in refs[k : k + 2]] for k in (9, 11))
        for m in range(4):
            store_digits(left_refs[m][:, j], left_scratch, (slice(None), slice(256 * m, 256 * m + 256)))
            block = pl.multiple_of((m ^ shift) * 256, 256)
            store_digits(right_refs[m][:, j], right_scratch, (pl.ds(block, 256), slice(None)))
        sums = [
            [jnp.dot(left[...], right[...], preferred_element_type=jnp.float32) for right in right_scratch]
            for left in left_scratch
        ]
        value = reduced(sums[0][0]) * 128.0 + (sums[0][1] + sums[1][0])
        value = reduced(reduced(value) * 128.0 + sums[1][1])
        out_ref[:, j] = to_wire(value).reshape(16, 16, 256)


def whole(shape):
    return pl.BlockSpec(shape, lambda i: (0,) * len(shape))


def params(mebibytes=12):
    return pltpu.CompilerParams(dimension_semantics=("arbitrary",), vmem_limit_bytes=mebibytes * 1024 * 1024)


def cost(flops):
    return pl.CostEstimate(flops=flops // 8, bytes_accessed=1 << 16, transcendentals=0)


def pack(first, second):
    both = [(value + 64).astype(jnp.int16).reshape(2, 16, 16, 256) for value in (first, second)]
    return jnp.stack(both).transpose(2, 0, 1, 3, 4)


def parted(both):
    shape = both.shape[:1] + (both.shape[1] // 2,) + both.shape[2:]
    return pl.pallas_call(
        part_kernel,
        grid=(1,),
        out_shape=[jax.ShapeDtypeStruct(shape, jnp.int16)] * 2,
        in_specs=[whole(both.shape)],
        out_specs=[whole(shape)] * 2,
        compiler_params=params(4),
        cost_estimate=cost(1 << 20),
    )(both)


def spread(table, entries, pair):
    count = table.shape[0] // 32
    out_shape = (16, 2 * count, 16, 256)
    return pl.pallas_call(
        spread_kernel,
        grid=(1,),
        out_shape=jax.ShapeDtypeStruct(out_shape, jnp.int16),
        in_specs=[whole(table.shape), pl.BlockSpec((8, 2, 2, 16, 256), lambda i: (pair, 0, 0, 0, 0))],
        out_specs=whole(out_shape),
        compiler_params=params(),
        cost_estimate=cost(4 * 2 * 64 * table.shape[0] * table.shape[1] * 256),
    )(table, entries)


def middle(table, values):
    out_shape = (16, POINTS // 16, 16, 256)
    return pl.pallas_call(
        middle_kernel,
        grid=(1,),
        out_shape=jax.ShapeDtypeStruct(out_shape, jnp.int16),
        in_specs=[whole(table.shape), whole(values.shape)],
        out_specs=whole(out_shape),
        compiler_params=params(),
        cost_estimate=cost(2 * 2 * 64 * table.shape[0] * table.shape[1] * 256),
        name="middle",
    )(table, values)


def final(table, values):
    out_shape = (COEFS, 16, 256)
    return pl.pallas_call(
        final_kernel,
        grid=(1,),
        out_shape=jax.ShapeDtypeStruct(out_shape, jnp.float32),
        in_specs=[whole(table.shape), whole(values.shape)],
        out_specs=whole(out_shape),
        compiler_params=params(),
        cost_estimate=cost(2 * 2 * 64 * table.shape[0] * table.shape[1] * 256),
        name="final",
    )(table, values)


def product(shift, left, right, aliases):
    shape = left[0].shape
    return pl.pallas_call(
        product_kernel,
        grid=(1,),
        out_shape=jax.ShapeDtypeStruct(shape, jnp.int16),
        in_specs=[pl.BlockSpec(memory_space=pltpu.SMEM)] + [whole(shape)] * 8,
        out_specs=whole(shape),
        scratch_shapes=[pltpu.VMEM((shape[1], 256, 1024), jnp.bfloat16)] * 2
        + [pltpu.VMEM((shape[1], 1024, 256), jnp.bfloat16)] * 2,
        input_output_aliases=aliases,
        compiler_params=params(20),
        cost_estimate=cost(shape[1] * 3 * 2 * 256 * 256 * 1024),
    )(shift, *left, *right)


def exchange(value):
    return lax.all_to_all(value, "pt", split_axis=0, concat_axis=0, tiled=True)


def swapped(value, axis, bits):
    return lax.ppermute(value, axis, [(i, i ^ bits) for i in range(4)])


def along_columns(value):
    return [value] + [swapped(value, "col", m) for m in (1, 2, 3)]


def along_rows(value):
    across = swapped(value, "row", 2)
    return [value, swapped(value, "row", 1), across, swapped(across, "row", 1)]


def local(first_factors, second_factors):
    forward_two = powers(4 * DEG, POINTS, 2 * DEG)
    spread_one = digit_table(powers(2 * DEG, 2 * DEG, DEG))
    spread_two = digit_table(forward_two[:, :DEG])
    lift = forward_two[:, :DEG] @ powers(2 * DEG, 2 * DEG, 2 * DEG, True)[DEG:] % modulus
    back = matrix_inverse(powers(4 * DEG, POINTS, POINTS))
    shift = (lax.axis_index("row") ^ lax.axis_index("col")).astype(jnp.int32).reshape(1)

    entries = exchange(pack(first_factors, second_factors))
    at_one = exchange(spread(spread_one, entries, 1))
    to_two = spread(spread_two, entries, 0)
    left_one, right_one = parted(at_one)
    left_one, right_one = along_columns(left_one), along_rows(right_one)
    to_two, at_one = lax.optimization_barrier((to_two, at_one))
    at_two = exchange(to_two)
    products_one = product(shift, left_one, right_one, {})
    products_one, at_two = lax.optimization_barrier((products_one, at_two))
    returned = exchange(products_one)
    left_two, right_two = parted(at_two)
    left_two, right_two = along_columns(left_two), along_rows(right_two)
    to_lower = middle(digit_table(lift), returned)
    upper = along_columns(product(shift, left_two, right_two, {1: 0}))
    lower = along_rows(exchange(to_lower))
    products_two = exchange(product(shift, upper, lower, {1: 0}))
    return final(digit_table(back), products_two)


def solution(mesh):
    in_specs = (P("pt", "row", "col"), P("pt", "row", "col"))
    out_specs = P(None, ("row", "pt"), "col")
    return jax.shard_map(local, mesh=mesh, in_specs=in_specs, out_specs=out_specs, check_vma=False)
```

```python
import jax
import jax.numpy as jnp
import numpy as np
from jax import lax
from jax.experimental import pallas as pl
from jax.experimental.pallas import tpu as pltpu
from jax.sharding import PartitionSpec as P

DEG = 16
POINTS = 48
COEFS = 3 * DEG - 3

modulus = 12289
inverse_modulus = 1.0 / modulus


def primitive_root():
    for candidate in range(2, modulus):
        if pow(candidate, 6144, modulus) != 1 and pow(candidate, 4096, modulus) != 1:
            return candidate
    return 0


def powers(order, row_count, column_count, inverse=False):
    root = pow(primitive_root(), (modulus - 1) // order, modulus)
    scaling = 1
    if inverse:
        root = pow(root, modulus - 2, modulus)
        scaling = pow(order, modulus - 2, modulus)
    entries = [
        [pow(root, i * j % order, modulus) * scaling % modulus for j in range(column_count)]
        for i in range(row_count)
    ]
    return np.array(entries, dtype=np.int64)


def matrix_inverse(matrix):
    size = matrix.shape[0]
    work = np.concatenate([matrix % modulus, np.eye(size, dtype=np.int64)], axis=1)
    for k in range(size):
        pivot = k + int(np.nonzero(work[k:, k])[0][0])
        work[[k, pivot]] = work[[pivot, k]]
        work[k] = work[k] * pow(int(work[k, k]), modulus - 2, modulus) % modulus
        for i in range(size):
            if i != k:
                work[i] = (work[i] - work[i, k] * work[k]) % modulus
    return work[:, size:]


def centred(values):
    values = values % modulus
    return np.where(values > modulus // 2, values - modulus, values)


def table_digits(values):
    values = centred(values)
    high = (values + 64) >> 7
    return high, values - 128 * high


def digit_table(matrix):
    of_high, of_low = table_digits(128 * matrix), table_digits(matrix)
    parts = [np.concatenate([of_high[k], of_low[k]], 1) for k in range(2)]
    return jnp.asarray(np.concatenate(parts, 0), dtype=jnp.bfloat16)


def expanded(table_ref):
    rows, columns = table_ref.shape
    wide = (columns, 8 * columns)
    place = lax.broadcasted_iota(jnp.int32, wide, 1) // 8 == lax.broadcasted_iota(jnp.int32, wide, 0)
    spread = jnp.dot(table_ref[...], place.astype(jnp.bfloat16), preferred_element_type=jnp.float32)
    full = (rows, 8, 8 * columns)
    same = lax.broadcasted_iota(jnp.int32, full, 2) % 8 == lax.broadcasted_iota(jnp.int32, full, 1)
    table = jnp.where(same, jnp.broadcast_to(spread[:, None, :], full), 0.0)
    return table.reshape(8 * rows, 8 * columns).astype(jnp.bfloat16)


def reduced(value):
    return value - jnp.floor(value * inverse_modulus + 0.5) * float(modulus)


def mixed(table, slots):
    inputs = slots.shape[0]
    half_rows = table.shape[0] // 2
    outputs = half_rows // 8
    halves = []
    for h in range(2):
        digits = jnp.concatenate(digits_of(slots[:, 8 * h : 8 * h + 8, :].reshape(inputs * 8, 256)), 0)
        sums = jnp.dot(table, digits, preferred_element_type=jnp.float32)
        top, bottom = sums[:half_rows], sums[half_rows:]
        quotient = jnp.floor(top * (128.0 * inverse_modulus) + bottom * inverse_modulus + 0.5)
        value = (top - 96.0 * quotient) * 128.0 + (bottom - quotient)
        halves.append(value.reshape(outputs, 8, 256))
    return jnp.concatenate(halves, axis=1)


def digits_of(wire):
    wire = wire.astype(jnp.int32)
    high = (wire >> 7).astype(jnp.float32).astype(jnp.bfloat16)
    low = (wire & 127).astype(jnp.float32).astype(jnp.bfloat16)
    return high, low - jnp.asarray(64.0, jnp.bfloat16)


def to_wire(value):
    return (value + 64.0).astype(jnp.int32).astype(jnp.int16)


def part_kernel(in_ref, left_ref, right_ref):
    count = left_ref.shape[1]
    left_ref[...] = in_ref[:, :count]
    right_ref[...] = in_ref[:, count:]


def spread_kernel(table_ref, in_ref, out_ref):
    count = out_ref.shape[1] // 2
    table = expanded(table_ref)
    for a in range(2):
        slots = in_ref[:, a].astype(jnp.int32).reshape(16, 16, 256)
        value = to_wire(mixed(table, slots))
        out_ref[:, a * count : (a + 1) * count] = value.reshape(16, count, 16, 256)


def middle_kernel(table_ref, in_ref, out_ref):
    slots = in_ref[...].astype(jnp.int32).reshape(-1, 16, 256)
    out_ref[...] = to_wire(mixed(expanded(table_ref), slots)).reshape(out_ref.shape)


def final_kernel(table_ref, in_ref, out_ref):
    slots = in_ref[...].astype(jnp.int32).reshape(-1, 16, 256)
    value = mixed(expanded(table_ref), slots)[:COEFS]
    value = jnp.where(value < 0.0, value + float(modulus), value)
    out_ref[...] = value / float(modulus)


def product_kernel(row_ref, column_ref, *refs):
    row, column = row_ref[0], column_ref[0]
    ringed = len(refs) > 13
    left_refs, right_refs, out_ref = refs[:-9], refs[-9:-5], refs[-5]

    def store_digits(piece, scratch, place):
        high, low = digits_of(piece.reshape(-1, 256))
        for part, ref in zip((high, low), scratch):
            ref[place] = part

    for j in range(out_ref.shape[1]):
        left_scratch, right_scratch = ([ref.at[j] for ref in group] for group in (refs[-4:-2], refs[-2:]))
        done = 0
        for ref in left_refs:
            rows, block = 16 * ref.shape[0], 256 * (done // 256)
            place = (slice(done % 256, done % 256 + rows), slice(block, block + 256))
            store_digits(ref[:, j], left_scratch, place)
            done += rows
        for m, ref in enumerate(right_refs):
            block = ((row ^ m) - column) & 3 if ringed else row ^ column ^ m
            block = pl.multiple_of(block * 256, 256)
            store_digits(ref[:, j], right_scratch, (pl.ds(block, 256), slice(None)))
        sums = [
            [jnp.dot(left[...], right[...], preferred_element_type=jnp.float32) for right in right_scratch]
            for left in left_scratch
        ]
        value = reduced(sums[0][0]) * 128.0 + (sums[0][1] + sums[1][0])
        value = reduced(reduced(value) * 128.0 + sums[1][1])
        out_ref[:, j] = to_wire(value).reshape(16, 16, 256)


def halves_kernel(first_ref, second_ref, low_ref, high_ref):
    low_ref[...] = first_ref[...]
    high_ref[...] = second_ref[...]


def whole(shape):
    return pl.BlockSpec(shape, lambda i: (0,) * len(shape))


def params(mebibytes=12):
    return pltpu.CompilerParams(dimension_semantics=("arbitrary",), vmem_limit_bytes=mebibytes * 1024 * 1024)


def cost(flops):
    return pl.CostEstimate(flops=flops // 8, bytes_accessed=1 << 16, transcendentals=0)


def pack(first, second):
    both = [(value + 64).astype(jnp.int16).reshape(2, 16, 16, 256) for value in (first, second)]
    return jnp.stack(both).transpose(2, 0, 1, 3, 4)


def parted(both):
    shape = both.shape[:1] + (both.shape[1] // 2,) + both.shape[2:]
    return pl.pallas_call(
        part_kernel,
        grid=(1,),
        out_shape=[jax.ShapeDtypeStruct(shape, jnp.int16)] * 2,
        in_specs=[whole(both.shape)],
        out_specs=[whole(shape)] * 2,
        compiler_params=params(4),
        cost_estimate=cost(1 << 20),
    )(both)


def spread(table, entries, pair):
    count = table.shape[0] // 32
    out_shape = (16, 2 * count, 16, 256)
    return pl.pallas_call(
        spread_kernel,
        grid=(1,),
        out_shape=jax.ShapeDtypeStruct(out_shape, jnp.int16),
        in_specs=[whole(table.shape), pl.BlockSpec((8, 2, 2, 16, 256), lambda i: (pair, 0, 0, 0, 0))],
        out_specs=whole(out_shape),
        compiler_params=params(),
        cost_estimate=cost(4 * 2 * 64 * table.shape[0] * table.shape[1] * 256),
    )(table, entries)


def middle(table, values):
    out_shape = (16, POINTS // 16, 16, 256)
    return pl.pallas_call(
        middle_kernel,
        grid=(1,),
        out_shape=jax.ShapeDtypeStruct(out_shape, jnp.int16),
        in_specs=[whole(table.shape), whole(values.shape)],
        out_specs=whole(out_shape),
        compiler_params=params(),
        cost_estimate=cost(2 * 2 * 64 * table.shape[0] * table.shape[1] * 256),
        name="middle",
    )(table, values)


def final(table, values):
    out_shape = (COEFS, 16, 256)
    return pl.pallas_call(
        final_kernel,
        grid=(1,),
        out_shape=jax.ShapeDtypeStruct(out_shape, jnp.float32),
        in_specs=[whole(table.shape), whole(values.shape)],
        out_specs=whole(out_shape),
        compiler_params=params(),
        cost_estimate=cost(2 * 2 * 64 * table.shape[0] * table.shape[1] * 256),
        name="final",
    )(table, values)


def halves(first, second):
    shape = (8,) + first.shape[1:]
    half = lambda k: pl.BlockSpec(shape, lambda i: (k, 0, 0, 0))
    return pl.pallas_call(
        halves_kernel,
        grid=(1,),
        out_shape=[jax.ShapeDtypeStruct(shape, jnp.int16)] * 2,
        in_specs=[half(0), half(1)],
        out_specs=[whole(shape)] * 2,
        compiler_params=params(4),
        cost_estimate=cost(1 << 20),
        name="halves",
    )(first, second)


def product(places, left, right, aliases):
    shape = left[0].shape
    return pl.pallas_call(
        product_kernel,
        grid=(1,),
        out_shape=jax.ShapeDtypeStruct(shape, jnp.int16),
        in_specs=[pl.BlockSpec(memory_space=pltpu.SMEM)] * 2 + [whole(piece.shape) for piece in (*left, *right)],
        out_specs=whole(shape),
        scratch_shapes=[pltpu.VMEM((shape[1], 256, 1024), jnp.bfloat16)] * 2
        + [pltpu.VMEM((shape[1], 1024, 256), jnp.bfloat16)] * 2,
        input_output_aliases=aliases,
        compiler_params=params(20),
        cost_estimate=cost(shape[1] * 3 * 2 * 256 * 256 * 1024),
    )(*places, *left, *right)


def exchange(value):
    return lax.all_to_all(value, "pt", split_axis=0, concat_axis=0, tiled=True)


def swapped(value, axis, bits):
    return lax.ppermute(value, axis, [(i, i ^ bits) for i in range(4)])


def along_columns(value):
    return [value] + [swapped(value, "col", m) for m in (1, 2, 3)]


def round_columns(value):
    def moved(piece, step):
        return lax.ppermute(piece, "col", [(i, (i + step) % 4) for i in range(4)])

    before, after = moved(value, 1), moved(value, 3)
    low, high = halves(before, after)
    return [value, after, moved(low, 1), moved(high, 3), before]


def along_rows(value):
    across = swapped(value, "row", 2)
    return [value, swapped(value, "row", 1), across, swapped(across, "row", 1)]


def local(first_factors, second_factors):
    forward_two = powers(4 * DEG, POINTS, 2 * DEG)
    spread_one = digit_table(powers(2 * DEG, 2 * DEG, DEG))
    spread_two = digit_table(forward_two[:, :DEG])
    lift = forward_two[:, :DEG] @ powers(2 * DEG, 2 * DEG, 2 * DEG, True)[DEG:] % modulus
    back = matrix_inverse(powers(4 * DEG, POINTS, POINTS))
    places = [lax.axis_index(axis).astype(jnp.int32).reshape(1) for axis in ("row", "col")]

    entries = exchange(pack(first_factors, second_factors))
    at_one = exchange(spread(spread_one, entries, 1))
    to_two = spread(spread_two, entries, 0)
    left_one, right_one = parted(at_one)
    left_one, right_one = along_columns(left_one), along_rows(right_one)
    to_two, at_one = lax.optimization_barrier((to_two, at_one))
    at_two = exchange(to_two)
    products_one = product(places, left_one, right_one, {})
    products_one, at_two = lax.optimization_barrier((products_one, at_two))
    returned = exchange(products_one)
    left_two, right_two = parted(at_two)
    left_two, right_two = along_columns(left_two), along_rows(right_two)
    to_lower = middle(digit_table(lift), returned)
    upper = round_columns(product(places, left_two, right_two, {2: 0}))
    lower = along_rows(exchange(to_lower))
    products_two = exchange(product(places, upper, lower, {2: 0}))
    return final(digit_table(back), products_two)


def solution(mesh):
    in_specs = (P("pt", "row", "col"), P("pt", "row", "col"))
    out_specs = P(None, ("row", "pt"), "col")
    return jax.shard_map(local, mesh=mesh, in_specs=in_specs, out_specs=out_specs, check_vma=False)
```
